256 devices in a mesh: gx: 8 (over z_hi, core), gy: 4 (over y), gz: 8 (over z_lo, x).
Axes of the slice: x: 4, y: 4, z: 8 (z_hi: 4, z_lo: 2; z = z_hi * 2 + z_lo), core: 2. Of those that a mesh axis runs over, the one named last changes fastest.
Arguments:
- field: float32 [256, 1024, 512], P('gz', 'gx', 'gy'), may hold values from -48 to 48
- factor_a: float32 [1024, 1024], replicated, may hold values from -0.5 to 3.5
- factor_b: float32 [512, 512], replicated, may hold values from -0.5 to 3.5
- factor_c: float32 [256, 256], replicated, may hold values from -0.5 to 3.5
Outputs:
- propagated: float32 [256, 1024, 512], P('gz', 'gx', 'gy')
The draws below stay inside these ranges and needn't reach their ends.
All inputs are finite; a program needn't handle non-finite values.
Results may differ from the reference program's by a relative error of at most 0.00007.
Values sent between devices are 32-bit elements; how exact they have to be, the bound alone decides.
A program may use at most 64 MiB of HBM per device.

```python
import math
import jax
import jax.numpy as jnp
from jax import lax

N1 = 1024
N2 = 512
N3 = 256


def draw_field(key, part):
    keys = jax.random.split(jax.random.fold_in(key, 10), 4)
    spread = math.log(2.2)
    rising = 0.5 * math.log(3.0)
    scale_three = jnp.exp(jax.random.uniform(keys[0], (N3,), jnp.float32, 0.0, spread) + rising * jnp.arange(N3, dtype=jnp.float32) / N3)
    scale_one = jnp.exp(jax.random.uniform(keys[1], (N1,), jnp.float32, 0.0, spread) + rising * jnp.arange(N1, dtype=jnp.float32) / N1)
    scale_two = jnp.exp(jax.random.uniform(keys[2], (N2,), jnp.float32, 0.0, spread) + rising * jnp.arange(N2, dtype=jnp.float32) / N2)
    noise = jax.random.truncated_normal(keys[3], -6.0, 6.0, (N3, N1, N2), jnp.float32)
    values = 0.25 * noise * scale_three[:, None, None] * scale_one[None, :, None] * scale_two[None, None, :]
    return jnp.clip(values, -48.0, 48.0)


def make_factor(key, order):
    keys = jax.random.split(key, 2)
    diagonal = jnp.exp(jax.random.uniform(keys[0], (order,), jnp.float32, 0.0, math.log(3.0)))
    off_part = jax.random.truncated_normal(keys[1], -4.0, 4.0, (order, order), jnp.float32) * 0.6 * order ** (-0.5)
    return off_part + jnp.diag(diagonal)


def draw_factor_a(key, part):
    return make_factor(jax.random.fold_in(key, 11), N1)


def draw_factor_b(key, part):
    return make_factor(jax.random.fold_in(key, 12), N2)


def draw_factor_c(key, part):
    return make_factor(jax.random.fold_in(key, 13), N3)


def setup_inputs(seed: int = 0) -> dict:
    splits = jax.random.split(jax.random.key(seed), 5)
    field = draw_field(jax.random.fold_in(splits[4], 71), 0)
    factor_a = draw_factor_a(jax.random.fold_in(splits[4], 71), 0)
    factor_b = draw_factor_b(jax.random.fold_in(splits[4], 71), 0)
    factor_c = draw_factor_c(jax.random.fold_in(splits[4], 71), 0)
    return {"field": field, "factor_a": factor_a, "factor_b": factor_b, "factor_c": factor_c}


epsilon = 1e-06
target_ratio = 0.5

def apply_operator(tensor, factor_a, factor_b, factor_c):
    highest = lax.Precision.HIGHEST
    along_one = jnp.einsum('ip,kpj->kij', factor_a, tensor, precision=highest)
    along_two = jnp.einsum('kip,jp->kij', tensor, factor_b, precision=highest)
    along_three = jnp.einsum('kp,pij->kij', factor_c, tensor, precision=highest)
    return along_one + along_two + along_three

def reference(field, factor_a, factor_b, factor_c):
    first_term = apply_operator(field, factor_a, factor_b, factor_c)
    size_field = jnp.sum(field * field)
    size_first = jnp.sum(first_term * first_term)
    step = target_ratio * jnp.sqrt(size_field / (size_first + epsilon))
    second_term = apply_operator(first_term, factor_a, factor_b, factor_c)
    return field - step * first_term + step * step / 2.0 * second_term
```

```python
import functools

import jax
import jax.numpy as jnp
from jax import lax
from jax.experimental import pallas as pl
from jax.experimental.pallas import tpu as pltpu
from jax.sharding import PartitionSpec as P

MESH = pl.DeviceIdType.MESH
F32, BF16 = jnp.float32, jnp.bfloat16

epsilon = 1e-06
target_ratio = 0.5

GX, GY, GZ = 8, 4, 8
GROUP = GX * GZ
BK, BI, BJ = 32, 128, 128
N1, N2, N3 = 1024, 512, 256
KY = BK // GY
PHASES = 2


def split(x):
    hi = x.astype(BF16)
    return hi, (x - hi.astype(F32)).astype(BF16)


def dot(a, b):
    return jnp.dot(a, b, preferred_element_type=F32)


def dot_t(a, b):
    return lax.dot_general(a, b, (((1,), (1,)), ((), ())), preferred_element_type=F32)


def member(t, gx, gz):
    z, x, c = (gx // 2) * 2 + gz // 4, gz % 4, gx % 2
    m, rest = t // 8, t % 8
    odd = m % 2
    dz = odd * ((m + 1) // 2) + (1 - odd) * (8 - m // 2)
    z2 = (z + dz) % 8
    x2 = (x + rest // 2) % 4
    c2 = (c + rest) % 2
    return (z2 // 2) * 2 + c2, (z2 % 2) * 4 + x2


def kernel(
    ft, a_hbm, b_hbm, c_hbm, out,
    a_f, b_f, c_f, a_h, a_l, b_h, b_l, c_h, c_l,
    wide, s_one, s_two, x_h, x_l,
    one_home, two_home, b_home, w_home,
    line_f, line_b, line_s, line_w,
    norm_src, norm_y, norm_mid, norm_all,
    load_sem, zs_sem, zr_sem, ys_sem, yr_sem, ns_sem, nr_sem,
):
    gx, gy, gz = lax.axis_index("gx"), lax.axis_index("gy"), lax.axis_index("gz")
    mine = gx * GZ + gz

    loads = [
        pltpu.make_async_copy(src, dst, load_sem.at[n])
        for n, (src, dst) in enumerate(((c_hbm, c_f), (a_hbm, a_f), (b_hbm, b_f)))
    ]
    for copy in loads:
        copy.start()

    barrier = pltpu.get_barrier_semaphore()

    def greet(t, carry):
        px, pz = member(t, gx, gz)
        pl.semaphore_signal(barrier, inc=1, device_id={"gx": px, "gz": pz}, device_id_type=MESH)
        return carry

    lax.fori_loop(1, GROUP, greet, 0)
    for d in range(1, GY):
        pl.semaphore_signal(
            barrier, inc=1, device_id={"gy": (gy + d) % GY}, device_id_type=MESH
        )
    pl.semaphore_wait(barrier, GROUP - 1 + GY - 1)

    def to_wide(p):
        def send(t, carry):
            px, pz = member(t, gx, gz)
            pltpu.make_async_remote_copy(
                src_ref=ft.at[p * GROUP + px * GZ + pz],
                dst_ref=wide.at[p, pl.ds(gz * BK, BK), pl.ds(gx * BI, BI)],
                send_sem=zs_sem.at[p], recv_sem=zr_sem.at[p],
                device_id={"gx": px, "gz": pz}, device_id_type=MESH,
            ).start()
            return carry

        lax.fori_loop(1, GROUP, send, 0)
        pltpu.make_async_copy(
            ft.at[p * GROUP + mine],
            wide.at[p, pl.ds(gz * BK, BK), pl.ds(gx * BI, BI)],
            zr_sem.at[p],
        ).start()

    def to_home(n, src, dst, p):
        slot = PHASES * n + p

        def send(t, carry):
            px, pz = member(t, gx, gz)
            pltpu.make_async_remote_copy(
                src_ref=src.at[p, pl.ds(pz * BK, BK), pl.ds(px * BI, BI)],
                dst_ref=dst.at[p * GROUP + mine],
                send_sem=zs_sem.at[slot], recv_sem=zr_sem.at[slot],
                device_id={"gx": px, "gz": pz}, device_id_type=MESH,
            ).start()
            return carry

        lax.fori_loop(1, GROUP, send, 0)
        pltpu.make_async_copy(
            src.at[p, pl.ds(gz * BK, BK), pl.ds(gx * BI, BI)],
            dst.at[p * GROUP + mine],
            zr_sem.at[slot],
        ).start()

    def wait_z(slot, ref):
        pltpu.make_async_copy(ref, ref, zr_sem.at[slot]).wait()

    def to_line(slot, src, dst, j0, rows):
        for d in range(1, GY):
            py = (gy + d) % GY
            pltpu.make_async_remote_copy(
                src_ref=src.at[pl.ds(j0, rows), pl.ds(py * KY, KY), :],
                dst_ref=dst.at[pl.ds(gy * BJ + j0, rows)],
                send_sem=ys_sem.at[slot], recv_sem=yr_sem.at[slot],
                device_id={"gy": py}, device_id_type=MESH,
            ).start()
        pltpu.make_async_copy(
            src.at[pl.ds(j0, rows), pl.ds(gy * KY, KY), :],
            dst.at[pl.ds(gy * BJ + j0, rows)],
            yr_sem.at[slot],
        ).start()

    def from_line(slot, src, dst):
        for d in range(1, GY):
            py = (gy + d) % GY
            pltpu.make_async_remote_copy(
                src_ref=src.at[pl.ds(py * BJ, BJ)],
                dst_ref=dst.at[:, pl.ds(gy * KY, KY), :],
                send_sem=ys_sem.at[slot], recv_sem=yr_sem.at[slot],
                device_id={"gy": py}, device_id_type=MESH,
            ).start()
        pltpu.make_async_copy(
            src.at[pl.ds(gy * BJ, BJ)],
            dst.at[:, pl.ds(gy * KY, KY), :],
            yr_sem.at[slot],
        ).start()

    def wait_y(slot, ref):
        pltpu.make_async_copy(ref, ref, yr_sem.at[slot]).wait()

    to_wide(0)
    to_line(0, ft, line_f, 0, BJ)
    to_wide(1)

    for copy in loads:
        copy.wait()
    c_h[...], c_l[...] = split(c_f[...])
    b_h[...], b_l[...] = split(b_f[...])

    def split_a(n, carry):
        rows = pl.ds(pl.multiple_of(n * 128, 128), 128)
        a_h[rows, :], a_l[rows, :] = split(a_f[rows, :])
        return carry

    lax.fori_loop(0, N1 // 128, split_a, 0)

    def along_wide(src, dst, p):
        def cut(n, carry):
            rows = pl.ds(pl.multiple_of(n * 64, 64), 64)
            x_h[rows, :], x_l[rows, :] = split(src[p, rows, :])
            return carry

        lax.fori_loop(0, N3 // 64, cut, 0)

        def tile(n, carry):
            cols = pl.ds(pl.multiple_of(n * 256, 256), 256)
            a_hi, a_lo = a_h[cols, :], a_l[cols, :]
            total = dot_t(x_h[...], a_hi) + dot_t(x_l[...], a_hi) + dot_t(x_h[...], a_lo)
            xh, xl = x_h[:, cols], x_l[:, cols]
            total = total + dot(c_h[...], xh) + dot(c_l[...], xh) + dot(c_h[...], xl)
            dst[p, :, cols] = total
            return carry

        lax.fori_loop(0, N1 // 256, tile, 0)

    def along_line(src, put):
        flat = src.reshape(N2 * KY, BI)

        def pair(q, carry):
            cols = [flat[pl.ds(2 * q + e, N2, stride=KY), :] for e in range(2)]
            xh, xl = split(jnp.concatenate(cols, axis=1))
            total = dot(b_h[...], xh) + dot(b_l[...], xh) + dot(b_h[...], xl)
            for e in range(2):
                put(pl.ds(2 * q + e, N2, stride=KY), total[:, e * BI:(e + 1) * BI])
            return carry

        lax.fori_loop(0, KY // 2, pair, 0)

    flat_b, flat_w = line_b.reshape(N2 * KY, BI), line_w.reshape(N2 * KY, BI)

    def put_b(rows, value):
        flat_b[rows, :] = value

    def put_w(rows, value):
        flat_w[rows, :] = value

    def add_w(rows, value):
        flat_w[rows, :] = flat_w[rows, :] + 2.0 * value

    wait_z(0, wide.at[0])
    along_wide(wide, s_one, 0)
    to_home(1, s_one, one_home, 0)

    wait_y(0, line_f)
    along_line(line_f, put_b)
    from_line(1, line_b, b_home)
    along_wide(s_one, s_two, 0)
    along_line(line_b, put_w)

    wait_z(1, wide.at[1])
    along_wide(wide, s_one, 1)
    to_home(1, s_one, one_home, 1)
    to_home(2, s_two, two_home, 0)
    along_wide(s_one, s_two, 1)

    def squares(read):
        def add(n, carry):
            v = read(pl.ds(n * 8, 8))
            return carry + jnp.sum(v * v, axis=(0, 1)).reshape(1, BI)

        return add

    zero = jnp.zeros((1, BI), F32)
    of_field = lax.fori_loop(0, BJ // 8, squares(lambda r: ft[r]), zero)
    wait_y(1, b_home)

    wait_z(2, one_home.at[pl.ds(0, GROUP)])
    to_line(2, one_home, line_s, 0, GROUP)
    first = squares(lambda r: one_home[r] + b_home[r])
    of_first = lax.fori_loop(0, GROUP // 8, first, zero)
    wait_z(3, one_home.at[pl.ds(GROUP, GROUP)])
    to_line(3, one_home, line_s, GROUP, GROUP)
    of_first = lax.fori_loop(GROUP // 8, BJ // 8, first, of_first)

    lane = lax.broadcasted_iota(jnp.int32, (1, BI), 1)
    norm_src[0] = jnp.where(lane == 0, jnp.sum(of_field), jnp.sum(of_first))

    def send_norm_y():
        for d in range(1, GY):
            pltpu.make_async_remote_copy(
                src_ref=norm_src, dst_ref=norm_y.at[pl.ds(gy, 1)],
                send_sem=ns_sem.at[0], recv_sem=nr_sem.at[0],
                device_id={"gy": (gy + d) % GY}, device_id_type=MESH,
            ).start()
        pltpu.make_async_copy(norm_src, norm_y.at[pl.ds(gy, 1)], nr_sem.at[0]).start()

    send_norm_y()
    to_home(2, s_two, two_home, 1)
    pltpu.make_async_copy(norm_y, norm_y, nr_sem.at[0]).wait()
    norm_mid[0] = norm_y[0] + norm_y[1] + norm_y[2] + norm_y[3]

    def send_norm(t, carry):
        px, pz = member(t, gx, gz)
        pltpu.make_async_remote_copy(
            src_ref=norm_mid, dst_ref=norm_all.at[pl.ds(mine, 1)],
            send_sem=ns_sem.at[1], recv_sem=nr_sem.at[1],
            device_id={"gx": px, "gz": pz}, device_id_type=MESH,
        ).start()
        return carry

    lax.fori_loop(1, GROUP, send_norm, 0)
    pltpu.make_async_copy(norm_mid, norm_all.at[pl.ds(mine, 1)], nr_sem.at[1]).start()

    wait_y(2, line_s.at[pl.ds(0, N2 // 2)])
    wait_y(3, line_s.at[pl.ds(0, N2 // 2)])
    along_line(line_s, add_w)
    from_line(4, line_w, w_home)

    pltpu.make_async_copy(norm_all, norm_all, nr_sem.at[1]).wait()
    sums = jnp.sum(norm_all[...], axis=0)
    size_field = jnp.sum(jnp.where(lane == 0, sums, 0.0))
    size_first = jnp.sum(jnp.where(lane == 1, sums, 0.0))
    ratio = jnp.full((1, BI), size_field, F32) / (jnp.full((1, BI), size_first, F32) + epsilon)
    step = (target_ratio * jnp.sqrt(ratio)).reshape(1, 1, BI)
    half = step * step / 2.0

    wait_z(4, two_home.at[pl.ds(0, GROUP)])
    wait_y(4, w_home)

    def finish(n, carry):
        r = pl.ds(n * 4, 4)
        out[r] = (ft[r] - step * (one_home[r] + b_home[r])) + half * (two_home[r] + w_home[r])
        return carry

    lax.fori_loop(0, GROUP // 4, finish, 0)
    wait_z(5, two_home.at[pl.ds(GROUP, GROUP)])
    lax.fori_loop(GROUP // 4, BJ // 4, finish, 0)

    for slot in range(6):
        sent = ft.at[pl.ds(0, GROUP - 1)]
        pltpu.make_async_copy(sent, sent, zs_sem.at[slot]).wait()
    for slot, rows in ((0, 3 * BJ), (1, 3 * BJ), (2, 3 * GROUP), (3, 3 * GROUP), (4, 3 * BJ)):
        sent = line_f.at[pl.ds(0, rows)]
        pltpu.make_async_copy(sent, sent, ys_sem.at[slot]).wait()
    sent = norm_y.at[pl.ds(0, GY - 1)]
    pltpu.make_async_copy(sent, sent, ns_sem.at[0]).wait()
    sent = norm_all.at[pl.ds(0, GROUP - 1)]
    pltpu.make_async_copy(sent, sent, ns_sem.at[1]).wait()


def on_device(field, factor_a, factor_b, factor_c):
    turned = jnp.transpose(field, (2, 0, 1))
    home = (BJ, BK, BI)
    vmem = pltpu.VMEM
    dma = pltpu.SemaphoreType.DMA
    scratch = [
        vmem((N1, N1), F32), vmem((N2, N2), F32), vmem((N3, N3), F32),
        vmem((N1, N1), BF16), vmem((N1, N1), BF16),
        vmem((N2, N2), BF16), vmem((N2, N2), BF16),
        vmem((N3, N3), BF16), vmem((N3, N3), BF16),
        vmem((PHASES, N3, N1), F32), vmem((PHASES, N3, N1), F32), vmem((PHASES, N3, N1), F32),
        vmem((N3, N1), BF16), vmem((N3, N1), BF16),
        vmem(home, F32), vmem(home, F32), vmem(home, F32), vmem(home, F32),
        vmem((N2, KY, BI), F32), vmem((N2, KY, BI), F32),
        vmem((N2, KY, BI), F32), vmem((N2, KY, BI), F32),
        vmem((1, 1, BI), F32), vmem((GY, 1, BI), F32),
        vmem((1, 1, BI), F32), vmem((GROUP, 1, BI), F32),
        dma((3,)), dma((6,)), dma((6,)), dma((5,)), dma((5,)), dma((2,)), dma((2,)),
    ]
    result = pl.pallas_call(
        kernel,
        out_shape=jax.ShapeDtypeStruct(home, F32),
        in_specs=[pl.BlockSpec(memory_space=pltpu.VMEM)] + [pl.BlockSpec(memory_space=pl.ANY)] * 3,
        out_specs=pl.BlockSpec(memory_space=pltpu.VMEM),
        scratch_shapes=scratch,
        compiler_params=pltpu.CompilerParams(
            collective_id=0, has_side_effects=True, vmem_limit_bytes=60 * 1024 * 1024
        ),
        name="taylor",
    )(turned, factor_a, factor_b, factor_c)
    return jnp.transpose(result, (1, 2, 0))


def solution(mesh):
    return jax.shard_map(
        on_device, mesh=mesh, in_specs=(P("gz", "gx", "gy"), P(), P(), P()),
        out_specs=P("gz", "gx", "gy"), check_vma=False,
    )
```

```python
import functools

import jax
import jax.numpy as jnp
from jax import lax
from jax.experimental import pallas as pl
from jax.experimental.pallas import tpu as pltpu
from jax.sharding import PartitionSpec as P

MESH = pl.DeviceIdType.MESH
F32, BF16 = jnp.float32, jnp.bfloat16

epsilon = 1e-06
target_ratio = 0.5

GX, GY, GZ = 8, 4, 8
GROUP = GX * GZ
BK, BI, BJ = 32, 128, 128
N1, N2, N3 = 1024, 512, 256
KY = BK // GY
PHASES = 2
SIDES = 2
HALF = GROUP // SIDES


def split(x):
    hi = x.astype(BF16)
    return hi, (x - hi.astype(F32)).astype(BF16)


def dot(a, b):
    return jnp.dot(a, b, preferred_element_type=F32)


def dot_t(a, b):
    return lax.dot_general(a, b, (((1,), (1,)), ((), ())), preferred_element_type=F32)


def member(t, gx, gz):
    z, x, c = (gx // 2) * 2 + gz // 4, gz % 4, gx % 2
    m, rest = t // 8, t % 8
    odd = m % 2
    dz = odd * ((m + 1) // 2) + (1 - odd) * (8 - m // 2)
    z2 = (z + dz) % 8
    x2 = (x + rest // 2) % 4
    c2 = (c + rest) % 2
    return (z2 // 2) * 2 + c2, (z2 % 2) * 4 + x2


def device_at(z, x, c):
    z, x, c = z % 8, x % 4, c % 2
    return (z // 2) * 2 + c, (z % 2) * 4 + x


def kernel(
    field, a_hbm, b_hbm, c_hbm, out,
    ft, b_f, c_f, a_h, a_l, b_h, b_l, c_h, c_l,
    wide, s_one, s_two, x_h, x_l,
    one_home, two_home, b_home, w_home,
    line_f, line_b, line_s, line_w,
    norm_src, norm_y, norm_mid, norm_all,
    load_sem, zs_sem, zr_sem, ys_sem, yr_sem, ns_sem, nr_sem,
):
    gx, gy, gz = lax.axis_index("gx"), lax.axis_index("gy"), lax.axis_index("gz")
    mine = gx * GZ + gz
    z, x, c = (gx // 2) * 2 + gz // 4, gz % 4, gx % 2

    pieces = [(c_hbm, c_f), (b_hbm, b_f)]
    pieces += [(a_hbm.at[pl.ds(n * N3, N3)], s_two.at[n]) for n in range(N1 // N3)]
    loads = [
        pltpu.make_async_copy(src, dst, load_sem.at[n]) for n, (src, dst) in enumerate(pieces)
    ]
    for copy in loads:
        copy.start()

    barrier = pltpu.get_barrier_semaphore()

    def greet(t, carry):
        px, pz = member(t, gx, gz)
        pl.semaphore_signal(barrier, inc=1, device_id={"gx": px, "gz": pz}, device_id_type=MESH)
        return carry

    lax.fori_loop(1, GROUP, greet, 0)
    for d in range(1, GY):
        pl.semaphore_signal(
            barrier, inc=1, device_id={"gy": (gy + d) % GY}, device_id_type=MESH
        )

    flat_ft = ft.reshape(BJ * BK, BI)

    def turn(k, carry):
        flat_ft[pl.ds(k, BJ, stride=BK), :] = field[k].T
        return carry

    lax.fori_loop(0, BK, turn, 0)
    pl.semaphore_wait(barrier, GROUP - 1 + GY - 1)

    def to_near(p, side):
        sign = 1 - 2 * side

        def place(u):
            up = sign * (u // 8)
            px, pz = device_at(z + up, x + u // 2, c + u)
            ox, oz = device_at(z + up - side, x + u // 2, c + u)
            src = ft.at[p * GROUP + ox * GZ + oz]
            dst = wide.at[2 * p + side, pl.ds(gz * BK, BK), pl.ds(gx * BI, BI)]
            return px, pz, src, dst

        def send(u, carry):
            px, pz, src, dst = place(u)
            pltpu.make_async_remote_copy(
                src_ref=src, dst_ref=dst,
                send_sem=zs_sem.at[2 * p + side], recv_sem=zr_sem.at[2 * p + side],
                device_id={"gx": px, "gz": pz}, device_id_type=MESH,
            ).start()
            return carry

        lax.fori_loop(1, HALF, send, 0)
        _, _, src, dst = place(0)
        pltpu.make_async_copy(src, dst, zr_sem.at[2 * p + side]).start()

    def swap(p, side):
        sign = 1 - 2 * side
        px, pz = device_at(z + sign, x, c)
        for n in range(4):
            from_z = (z - sign * n) % 8
            rows = pl.ds((from_z % 2) * (N3 // 2), N3 // 2)
            cols = pl.ds((from_z // 2) * (N1 // 4), N1 // 4)
            pltpu.make_async_remote_copy(
                src_ref=wide.at[2 * p + side, rows, cols],
                dst_ref=wide.at[2 * p + 1 - side, rows, cols],
                send_sem=zs_sem.at[4 + 2 * p + side], recv_sem=zr_sem.at[4 + 2 * p + 1 - side],
                device_id={"gx": px, "gz": pz}, device_id_type=MESH,
            ).start()

    def to_home(n, src, dst, p, side):
        sign = 1 - 2 * side
        ox, oz = device_at(z - side, x, c)
        row = p * GROUP + ox * GZ + oz

        def place(u):
            px, pz = device_at(z - sign * (u // 8), x + u // 2, c + u)
            return px, pz, src.at[2 * p + side, pl.ds(pz * BK, BK), pl.ds(px * BI, BI)]

        def send(u, carry):
            px, pz, block = place(u)
            pltpu.make_async_remote_copy(
                src_ref=block, dst_ref=dst.at[row],
                send_sem=zs_sem.at[8 + 4 * n + 2 * p + side], recv_sem=zr_sem.at[8 + 2 * n + p],
                device_id={"gx": px, "gz": pz}, device_id_type=MESH,
            ).start()
            return carry

        lax.fori_loop(1, HALF, send, 0)
        _, _, block = place(0)
        pltpu.make_async_copy(block, dst.at[row], zr_sem.at[8 + 2 * n + p]).start()

    def wait_z(slot, ref):
        pltpu.make_async_copy(ref, ref, zr_sem.at[slot]).wait()

    def wait_half(slot):
        wait_z(slot, wide.at[0, pl.ds(0, N3 // 2)])

    def to_line(slot, src, dst, j0, rows):
        for d in range(1, GY):
            py = (gy + d) % GY
            pltpu.make_async_remote_copy(
                src_ref=src.at[pl.ds(j0, rows), pl.ds(py * KY, KY), :],
                dst_ref=dst.at[pl.ds(gy * BJ + j0, rows)],
                send_sem=ys_sem.at[slot], recv_sem=yr_sem.at[slot],
                device_id={"gy": py}, device_id_type=MESH,
            ).start()
        pltpu.make_async_copy(
            src.at[pl.ds(j0, rows), pl.ds(gy * KY, KY), :],
            dst.at[pl.ds(gy * BJ + j0, rows)],
            yr_sem.at[slot],
        ).start()

    def from_line(slot, src, dst):
        for d in range(1, GY):
            py = (gy + d) % GY
            pltpu.make_async_remote_copy(
                src_ref=src.at[pl.ds(py * BJ, BJ)],
                dst_ref=dst.at[:, pl.ds(gy * KY, KY), :],
                send_sem=ys_sem.at[slot], recv_sem=yr_sem.at[slot],
                device_id={"gy": py}, device_id_type=MESH,
            ).start()
        pltpu.make_async_copy(
            src.at[pl.ds(gy * BJ, BJ)],
            dst.at[:, pl.ds(gy * KY, KY), :],
            yr_sem.at[slot],
        ).start()

    def wait_y(slot, ref):
        pltpu.make_async_copy(ref, ref, yr_sem.at[slot]).wait()

    for side in range(SIDES):
        to_near(0, side)
    to_line(0, ft, line_f, 0, BJ)
    for side in range(SIDES):
        to_near(1, side)

    for copy in loads:
        copy.wait()
    c_h[...], c_l[...] = split(c_f[...])
    b_h[...], b_l[...] = split(b_f[...])

    def split_a(n, carry):
        rows = pl.ds(pl.multiple_of(n * 128, 128), 128)
        part = pl.ds(pl.multiple_of((n % 2) * 128, 128), 128)
        a_h[rows, :], a_l[rows, :] = split(s_two[n // 2, part, :])
        return carry

    lax.fori_loop(0, N1 // 128, split_a, 0)

    def along_wide(src, dst, p):
        def cut(n, carry):
            rows = pl.ds(pl.multiple_of(n * 64, 64), 64)
            x_h[rows, :], x_l[rows, :] = split(src[p, rows, :])
            return carry

        lax.fori_loop(0, N3 // 64, cut, 0)

        def tile(n, carry):
            cols = pl.ds(pl.multiple_of(n * 256, 256), 256)
            a_hi, a_lo = a_h[cols, :], a_l[cols, :]
            total = dot_t(x_h[...], a_hi) + dot_t(x_l[...], a_hi) + dot_t(x_h[...], a_lo)
            xh, xl = x_h[:, cols], x_l[:, cols]
            total = total + dot(c_h[...], xh) + dot(c_l[...], xh) + dot(c_h[...], xl)
            dst[p, :, cols] = total
            return carry

        lax.fori_loop(0, N1 // 256, tile, 0)

    def along_line(src, put):
        flat = src.reshape(N2 * KY, BI)

        def pair(q, carry):
            cols = [flat[pl.ds(2 * q + e, N2, stride=KY), :] for e in range(2)]
            xh, xl = split(jnp.concatenate(cols, axis=1))
            total = dot(b_h[...], xh) + dot(b_l[...], xh) + dot(b_h[...], xl)
            for e in range(2):
                put(pl.ds(2 * q + e, N2, stride=KY), total[:, e * BI:(e + 1) * BI])
            return carry

        lax.fori_loop(0, KY // 2, pair, 0)

    flat_b, flat_w = line_b.reshape(N2 * KY, BI), line_w.reshape(N2 * KY, BI)

    def put_b(rows, value):
        flat_b[rows, :] = value

    def put_w(rows, value):
        flat_w[rows, :] = value

    def add_w(rows, value):
        flat_w[rows, :] = flat_w[rows, :] + 2.0 * value

    for side in range(SIDES):
        wait_half(side)
        swap(0, side)

    wait_y(0, line_f)
    along_line(line_f, put_b)
    from_line(1, line_b, b_home)
    along_line(line_b, put_w)

    for side in range(SIDES):
        wait_half(2 + side)
        swap(1, side)

    for p in range(PHASES):
        for side in range(SIDES):
            wait_half(4 + 2 * p + side)
            along_wide(wide, s_one, 2 * p + side)
            to_home(0, s_one, one_home, p, side)
    for side in range(SIDES):
        along_wide(s_one, s_two, side)
        to_home(1, s_two, two_home, 0, side)
    for side in range(SIDES):
        along_wide(s_one, s_two, 2 + side)

    def squares(read):
        def add(n, carry):
            v = read(pl.ds(n * 8, 8))
            return carry + jnp.sum(v * v, axis=(0, 1)).reshape(1, BI)

        return add

    zero = jnp.zeros((1, BI), F32)
    of_field = lax.fori_loop(0, BJ // 8, squares(lambda r: ft[r]), zero)
    wait_y(1, b_home)

    wait_z(8, one_home.at[pl.ds(0, GROUP)])
    to_line(2, one_home, line_s, 0, GROUP)
    first = squares(lambda r: one_home[r] + b_home[r])
    of_first = lax.fori_loop(0, GROUP // 8, first, zero)
    wait_z(9, one_home.at[pl.ds(GROUP, GROUP)])
    to_line(3, one_home, line_s, GROUP, GROUP)
    of_first = lax.fori_loop(GROUP // 8, BJ // 8, first, of_first)

    lane = lax.broadcasted_iota(jnp.int32, (1, BI), 1)
    norm_src[0] = jnp.where(lane == 0, jnp.sum(of_field), jnp.sum(of_first))

    def send_norm_y():
        for d in range(1, GY):
            pltpu.make_async_remote_copy(
                src_ref=norm_src, dst_ref=norm_y.at[pl.ds(gy, 1)],
                send_sem=ns_sem.at[0], recv_sem=nr_sem.at[0],
                device_id={"gy": (gy + d) % GY}, device_id_type=MESH,
            ).start()
        pltpu.make_async_copy(norm_src, norm_y.at[pl.ds(gy, 1)], nr_sem.at[0]).start()

    send_norm_y()
    for side in range(SIDES):
        to_home(1, s_two, two_home, 1, side)
    pltpu.make_async_copy(norm_y, norm_y, nr_sem.at[0]).wait()
    norm_mid[0] = norm_y[0] + norm_y[1] + norm_y[2] + norm_y[3]

    def send_norm(t, carry):
        px, pz = member(t, gx, gz)
        pltpu.make_async_remote_copy(
            src_ref=norm_mid, dst_ref=norm_all.at[pl.ds(mine, 1)],
            send_sem=ns_sem.at[1], recv_sem=nr_sem.at[1],
            device_id={"gx": px, "gz": pz}, device_id_type=MESH,
        ).start()
        return carry

    lax.fori_loop(1, GROUP, send_norm, 0)
    pltpu.make_async_copy(norm_mid, norm_all.at[pl.ds(mine, 1)], nr_sem.at[1]).start()

    wait_y(2, line_s.at[pl.ds(0, N2 // 2)])
    wait_y(3, line_s.at[pl.ds(0, N2 // 2)])
    along_line(line_s, add_w)
    from_line(4, line_w, w_home)

    pltpu.make_async_copy(norm_all, norm_all, nr_sem.at[1]).wait()
    sums = jnp.sum(norm_all[...], axis=0)
    size_field = jnp.sum(jnp.where(lane == 0, sums, 0.0))
    size_first = jnp.sum(jnp.where(lane == 1, sums, 0.0))
    ratio = jnp.full((1, BI), size_field, F32) / (jnp.full((1, BI), size_first, F32) + epsilon)
    step = (target_ratio * jnp.sqrt(ratio)).reshape(1, 1, BI)
    half = step * step / 2.0

    wait_z(10, two_home.at[pl.ds(0, GROUP)])
    wait_y(4, w_home)

    def finish(n, carry):
        r = pl.ds(n * 4, 4)
        out[r] = (ft[r] - step * (one_home[r] + b_home[r])) + half * (two_home[r] + w_home[r])
        return carry

    lax.fori_loop(0, GROUP // 4, finish, 0)
    wait_z(11, two_home.at[pl.ds(GROUP, GROUP)])
    lax.fori_loop(GROUP // 4, BJ // 4, finish, 0)

    for slot in range(16):
        sent = wide.at[0, pl.ds(0, N3 // 2)] if 4 <= slot < 8 else ft.at[pl.ds(0, HALF - 1)]
        pltpu.make_async_copy(sent, sent, zs_sem.at[slot]).wait()
    for slot, rows in ((0, 3 * BJ), (1, 3 * BJ), (2, 3 * GROUP), (3, 3 * GROUP), (4, 3 * BJ)):
        sent = line_f.at[pl.ds(0, rows)]
        pltpu.make_async_copy(sent, sent, ys_sem.at[slot]).wait()
    sent = norm_y.at[pl.ds(0, GY - 1)]
    pltpu.make_async_copy(sent, sent, ns_sem.at[0]).wait()
    sent = norm_all.at[pl.ds(0, GROUP - 1)]
    pltpu.make_async_copy(sent, sent, ns_sem.at[1]).wait()


def on_device(field, factor_a, factor_b, factor_c):
    home = (BJ, BK, BI)
    vmem = pltpu.VMEM
    dma = pltpu.SemaphoreType.DMA
    scratch = [
        vmem(home, F32), vmem((N2, N2), F32), vmem((N3, N3), F32),
        vmem((N1, N1), BF16), vmem((N1, N1), BF16),
        vmem((N2, N2), BF16), vmem((N2, N2), BF16),
        vmem((N3, N3), BF16), vmem((N3, N3), BF16),
        vmem((4, N3, N1), F32), vmem((4, N3, N1), F32), vmem((4, N3, N1), F32),
        vmem((N3, N1), BF16), vmem((N3, N1), BF16),
        vmem(home, F32), vmem(home, F32), vmem(home, F32), vmem(home, F32),
        vmem((N2, KY, BI), F32), vmem((N2, KY, BI), F32),
        vmem((N2, KY, BI), F32), vmem((N2, KY, BI), F32),
        vmem((1, 1, BI), F32), vmem((GY, 1, BI), F32),
        vmem((1, 1, BI), F32), vmem((GROUP, 1, BI), F32),
        dma((6,)), dma((16,)), dma((12,)), dma((5,)), dma((5,)), dma((2,)), dma((2,)),
    ]
    result = pl.pallas_call(
        kernel,
        out_shape=jax.ShapeDtypeStruct(home, F32),
        in_specs=[pl.BlockSpec(memory_space=pltpu.VMEM)] + [pl.BlockSpec(memory_space=pl.ANY)] * 3,
        out_specs=pl.BlockSpec(memory_space=pltpu.VMEM),
        scratch_shapes=scratch,
        compiler_params=pltpu.CompilerParams(
            collective_id=0, has_side_effects=True, vmem_limit_bytes=60 * 1024 * 1024
        ),
        name="taylor",
    )(field, factor_a, factor_b, factor_c)
    return jnp.transpose(result, (1, 2, 0))


def solution(mesh):
    return jax.shard_map(
        on_device, mesh=mesh, in_specs=(P("gz", "gx", "gy"), P(), P(), P()),
        out_specs=P("gz", "gx", "gy"), check_vma=False,
    )
```

```python
import functools

import jax
import jax.numpy as jnp
from jax import lax
from jax.experimental import pallas as pl
from jax.experimental.pallas import tpu as pltpu
from jax.sharding import PartitionSpec as P

MESH = pl.DeviceIdType.MESH
F32, BF16 = jnp.float32, jnp.bfloat16

epsilon = 1e-06
target_ratio = 0.5

GX, GY, GZ = 8, 4, 8
GROUP = GX * GZ
BK, BI, BJ = 32, 128, 128
N1, N2, N3 = 1024, 512, 256
KY = BK // GY
PHASES = 2
SIDES = 2
HALF = GROUP // SIDES


def split(x):
    hi = x.astype(BF16)
    return hi, (x - hi.astype(F32)).astype(BF16)


def dot(a, b):
    return jnp.dot(a, b, preferred_element_type=F32)


def dot_t(a, b):
    return lax.dot_general(a, b, (((1,), (1,)), ((), ())), preferred_element_type=F32)


def member(t, gx, gz):
    z, x, c = (gx // 2) * 2 + gz // 4, gz % 4, gx % 2
    m, rest = t // 8, t % 8
    odd = m % 2
    dz = odd * ((m + 1) // 2) + (1 - odd) * (8 - m // 2)
    z2 = (z + dz) % 8
    x2 = (x + rest // 2) % 4
    c2 = (c + rest) % 2
    return (z2 // 2) * 2 + c2, (z2 % 2) * 4 + x2


def device_at(z, x, c):
    z, x, c = z % 8, x % 4, c % 2
    return (z // 2) * 2 + c, (z % 2) * 4 + x


def kernel(
    field, a_hbm, b_hbm, c_hbm, out,
    ft, b_f, c_f, a_h, a_l, b_h, b_l, c_h, c_l,
    wide, s_one, s_two, x_h, x_l,
    one_home, two_home, b_home, w_home,
    line_f, line_b, line_s, line_w,
    l_h, l_l, norm_src, norm_y, norm_mid, norm_all,
    load_sem, zs_sem, zr_sem, ys_sem, yr_sem, ns_sem, nr_sem,
):
    gx, gy, gz = lax.axis_index("gx"), lax.axis_index("gy"), lax.axis_index("gz")
    mine = gx * GZ + gz
    z, x, c = (gx // 2) * 2 + gz // 4, gz % 4, gx % 2

    pieces = [(c_hbm, c_f), (b_hbm, b_f)]
    pieces += [(a_hbm.at[pl.ds(n * N3, N3)], s_two.at[n]) for n in range(N1 // N3)]
    loads = [
        pltpu.make_async_copy(src, dst, load_sem.at[n]) for n, (src, dst) in enumerate(pieces)
    ]
    for copy in loads:
        copy.start()

    barrier = pltpu.get_barrier_semaphore()

    def greet(t, carry):
        px, pz = member(t, gx, gz)
        pl.semaphore_signal(barrier, inc=1, device_id={"gx": px, "gz": pz}, device_id_type=MESH)
        return carry

    lax.fori_loop(1, GROUP, greet, 0)
    for d in range(1, GY):
        pl.semaphore_signal(
            barrier, inc=1, device_id={"gy": (gy + d) % GY}, device_id_type=MESH
        )

    flat_ft = ft.reshape(BJ * BK, BI)

    def turn(k, carry):
        flat_ft[pl.ds(k, BJ, stride=BK), :] = field[k].T
        return carry

    lax.fori_loop(0, BK, turn, 0)
    pl.semaphore_wait(barrier, GROUP - 1 + GY - 1)

    def to_near(p, side):
        sign = 1 - 2 * side

        def place(u):
            up = sign * (u // 8)
            px, pz = device_at(z + up, x + u // 2, c + u)
            ox, oz = device_at(z + up - side, x + u // 2, c + u)
            src = ft.at[p * GROUP + ox * GZ + oz]
            dst = wide.at[2 * p + side, pl.ds(gz * BK, BK), pl.ds(gx * BI, BI)]
            return px, pz, src, dst

        def send(u, carry):
            px, pz, src, dst = place(u)
            pltpu.make_async_remote_copy(
                src_ref=src, dst_ref=dst,
                send_sem=zs_sem.at[2 * p + side], recv_sem=zr_sem.at[2 * p + side],
                device_id={"gx": px, "gz": pz}, device_id_type=MESH,
            ).start()
            return carry

        lax.fori_loop(1, HALF, send, 0)
        _, _, src, dst = place(0)
        pltpu.make_async_copy(src, dst, zr_sem.at[2 * p + side]).start()

    def swap(p, side):
        sign = 1 - 2 * side
        px, pz = device_at(z + sign, x, c)
        for n in range(4):
            from_z = (z - sign * n) % 8
            rows = pl.ds((from_z % 2) * (N3 // 2), N3 // 2)
            cols = pl.ds((from_z // 2) * (N1 // 4), N1 // 4)
            pltpu.make_async_remote_copy(
                src_ref=wide.at[2 * p + side, rows, cols],
                dst_ref=wide.at[2 * p + 1 - side, rows, cols],
                send_sem=zs_sem.at[4 + 2 * p + side], recv_sem=zr_sem.at[4 + 2 * p + 1 - side],
                device_id={"gx": px, "gz": pz}, device_id_type=MESH,
            ).start()

    def to_home(n, src, dst, p, side, k0=0, depth=BK, late=0):
        sign = 1 - 2 * side
        ox, oz = device_at(z - side, x, c)
        row = p * GROUP + ox * GZ + oz
        target = dst.at[row, pl.ds(k0, depth)]
        arrived = zr_sem.at[8 + 2 * n + p + 3 * late]

        def place(u):
            px, pz = device_at(z - sign * (u // 8), x + u // 2, c + u)
            block = src.at[2 * p + side, pl.ds(pz * BK + k0, depth), pl.ds(px * BI, BI)]
            return px, pz, block

        def send(u, carry):
            px, pz, block = place(u)
            pltpu.make_async_remote_copy(
                src_ref=block, dst_ref=target,
                send_sem=zs_sem.at[8 + 4 * n + 2 * p + side], recv_sem=arrived,
                device_id={"gx": px, "gz": pz}, device_id_type=MESH,
            ).start()
            return carry

        lax.fori_loop(1, HALF, send, 0)
        _, _, block = place(0)
        pltpu.make_async_copy(block, target, arrived).start()

    def wait_z(slot, ref):
        pltpu.make_async_copy(ref, ref, zr_sem.at[slot]).wait()

    def wait_half(slot):
        wait_z(slot, wide.at[0, pl.ds(0, N3 // 2)])

    def to_peer(slot, src, dst, j0, rows, py):
        pltpu.make_async_remote_copy(
            src_ref=src.at[pl.ds(j0, rows), pl.ds(py * KY, KY), :],
            dst_ref=dst.at[pl.ds(gy * BJ + j0, rows)],
            send_sem=ys_sem.at[slot], recv_sem=yr_sem.at[slot],
            device_id={"gy": py}, device_id_type=MESH,
        ).start()

    def to_line(slot, src, dst, j0, rows, peers=(1, 2, 3), own=True):
        for d in peers:
            to_peer(slot, src, dst, j0, rows, (gy + d) % GY)
        if own:
            pltpu.make_async_copy(
                src.at[pl.ds(j0, rows), pl.ds(gy * KY, KY), :],
                dst.at[pl.ds(gy * BJ + j0, rows)],
                yr_sem.at[slot],
            ).start()

    def from_line(slot, src, dst, d):
        py = (gy + d) % GY
        source, target = src.at[pl.ds(py * BJ, BJ)], dst.at[:, pl.ds(gy * KY, KY), :]
        if d:
            pltpu.make_async_remote_copy(
                src_ref=source, dst_ref=target,
                send_sem=ys_sem.at[slot], recv_sem=yr_sem.at[slot],
                device_id={"gy": py}, device_id_type=MESH,
            ).start()
        else:
            pltpu.make_async_copy(source, target, yr_sem.at[slot]).start()

    def wait_y(slot, ref):
        pltpu.make_async_copy(ref, ref, yr_sem.at[slot]).wait()

    for side in range(SIDES):
        to_near(0, side)
    to_line(0, ft, line_f, 0, BJ)
    for side in range(SIDES):
        to_near(1, side)

    for copy in loads:
        copy.wait()
    c_h[...], c_l[...] = split(c_f[...])
    b_h[...], b_l[...] = split(b_f[...])

    def split_a(n, carry):
        rows = pl.ds(pl.multiple_of(n * 128, 128), 128)
        part = pl.ds(pl.multiple_of((n % 2) * 128, 128), 128)
        a_h[rows, :], a_l[rows, :] = split(s_two[n // 2, part, :])
        return carry

    lax.fori_loop(0, N1 // 128, split_a, 0)

    def along_wide(src, dst, p):
        def cut(n, carry):
            rows = pl.ds(pl.multiple_of(n * 64, 64), 64)
            x_h[rows, :], x_l[rows, :] = split(src[p, rows, :])
            return carry

        lax.fori_loop(0, N3 // 64, cut, 0)

        def tile(n, carry):
            cols = pl.ds(pl.multiple_of(n * 256, 256), 256)
            a_hi, a_lo = a_h[cols, :], a_l[cols, :]
            total = dot_t(x_h[...], a_hi) + dot_t(x_l[...], a_hi) + dot_t(x_h[...], a_lo)
            xh, xl = x_h[:, cols], x_l[:, cols]
            total = total + dot(c_h[...], xh) + dot(c_l[...], xh) + dot(c_h[...], xl)
            dst[p, :, cols] = total
            return carry

        lax.fori_loop(0, N1 // 256, tile, 0)

    def cut_line(src, j0, rows):
        flat = src.reshape(N2 * KY, BI)
        to = pl.ds(j0, rows)

        def one(k, carry):
            cols = pl.ds(pl.multiple_of(k * BI, BI), BI)
            l_h[to, cols], l_l[to, cols] = split(flat[pl.ds(j0 * KY + k, rows, stride=KY), :])
            return carry

        lax.fori_loop(0, KY, one, 0)

    def line_rows(d, dst, add):
        j0 = pl.multiple_of((gy + d) % GY * BJ, BJ)
        flat = dst.reshape(N2 * KY, BI)
        b_hi, b_lo = b_h[pl.ds(j0, BJ), :], b_l[pl.ds(j0, BJ), :]

        def pair(q, carry):
            cols = pl.ds(pl.multiple_of(q * 2 * BI, 2 * BI), 2 * BI)
            xh, xl = l_h[:, cols], l_l[:, cols]
            total = dot(b_hi, xh) + dot(b_hi, xl) + dot(b_lo, xh)
            for e in range(2):
                rows = pl.ds(j0 * KY + 2 * q + e, BJ, stride=KY)
                part = total[:, e * BI:(e + 1) * BI]
                flat[rows, :] = flat[rows, :] + 2.0 * part if add else part
            return carry

        lax.fori_loop(0, KY // 2, pair, 0)

    for side in range(SIDES):
        wait_half(side)
        swap(0, side)

    wait_y(0, line_f)
    cut_line(line_f, 0, N2)
    for d in (1, 2, 3, 0):
        line_rows(d, line_b, False)
        from_line(1, line_b, b_home, d)
    cut_line(line_b, 0, N2)
    for d in range(GY):
        line_rows(d, line_w, False)

    for side in range(SIDES):
        wait_half(2 + side)
        swap(1, side)

    k_early, k_late = (1 - gy // 2) * (BK // 2), (gy // 2) * (BK // 2)
    for side in range(SIDES):
        wait_half(4 + side)
        along_wide(wide, s_one, side)
        to_home(0, s_one, one_home, 0, side)
    for side in range(SIDES):
        wait_half(6 + side)
        along_wide(wide, s_one, 2 + side)
    for side in range(SIDES):
        to_home(0, s_one, one_home, 1, side, k_early, BK // 2)
    for side in range(SIDES):
        to_home(0, s_one, one_home, 1, side, k_late, BK // 2, late=1)
    for side in range(SIDES):
        along_wide(s_one, s_two, side)
        to_home(1, s_two, two_home, 0, side)
    for side in range(SIDES):
        along_wide(s_one, s_two, 2 + side)

    def squares(read):
        def add(n, carry):
            v = read(pl.ds(n * 8, 8))
            return carry + jnp.sum(v * v, axis=(0, 1)).reshape(1, BI)

        return add

    zero = jnp.zeros((1, BI), F32)
    of_field = lax.fori_loop(0, BJ // 8, squares(lambda r: ft[r]), zero)
    wait_y(1, b_home)

    wait_z(8, one_home.at[pl.ds(0, GROUP)])
    to_line(2, one_home, line_s, 0, GROUP)
    first = squares(lambda r: one_home[r] + b_home[r])
    of_first = lax.fori_loop(0, GROUP // 8, first, zero)
    half_phase = one_home.at[pl.ds(0, GROUP), pl.ds(0, BK // 2)]
    wait_z(9, half_phase)
    for tile in range(2):
        py = (1 - gy // 2) * 2 + tile
        to_peer(3, one_home, line_s, GROUP, GROUP, py)
    wait_z(12, half_phase)
    to_peer(3, one_home, line_s, GROUP, GROUP, gy + 1 - 2 * (gy % 2))
    to_line(3, one_home, line_s, GROUP, GROUP, peers=())
    of_first = lax.fori_loop(GROUP // 8, BJ // 8, first, of_first)

    lane = lax.broadcasted_iota(jnp.int32, (1, BI), 1)
    norm_src[0] = jnp.where(lane == 0, jnp.sum(of_field), jnp.sum(of_first))

    def send_norm_y():
        for d in range(1, GY):
            pltpu.make_async_remote_copy(
                src_ref=norm_src, dst_ref=norm_y.at[pl.ds(gy, 1)],
                send_sem=ns_sem.at[0], recv_sem=nr_sem.at[0],
                device_id={"gy": (gy + d) % GY}, device_id_type=MESH,
            ).start()
        pltpu.make_async_copy(norm_src, norm_y.at[pl.ds(gy, 1)], nr_sem.at[0]).start()

    send_norm_y()
    for side in range(SIDES):
        to_home(1, s_two, two_home, 1, side)
    pltpu.make_async_copy(norm_y, norm_y, nr_sem.at[0]).wait()
    norm_mid[0] = norm_y[0] + norm_y[1] + norm_y[2] + norm_y[3]

    def send_norm(t, carry):
        px, pz = member(t, gx, gz)
        pltpu.make_async_remote_copy(
            src_ref=norm_mid, dst_ref=norm_all.at[pl.ds(mine, 1)],
            send_sem=ns_sem.at[1], recv_sem=nr_sem.at[1],
            device_id={"gx": px, "gz": pz}, device_id_type=MESH,
        ).start()
        return carry

    lax.fori_loop(1, GROUP, send_norm, 0)
    pltpu.make_async_copy(norm_mid, norm_all.at[pl.ds(mine, 1)], nr_sem.at[1]).start()

    wait_y(2, line_s.at[pl.ds(0, N2 // 2)])
    for d in range(GY):
        cut_line(line_s, d * BJ, GROUP)
    wait_y(3, line_s.at[pl.ds(0, N2 // 2)])
    for d in range(GY):
        cut_line(line_s, d * BJ + GROUP, GROUP)
    for d in (2, 1, 3, 0):
        line_rows(d, line_w, True)
        from_line(4, line_w, w_home, d)

    pltpu.make_async_copy(norm_all, norm_all, nr_sem.at[1]).wait()
    sums = jnp.sum(norm_all[...], axis=0)
    size_field = jnp.sum(jnp.where(lane == 0, sums, 0.0))
    size_first = jnp.sum(jnp.where(lane == 1, sums, 0.0))
    ratio = jnp.full((1, BI), size_field, F32) / (jnp.full((1, BI), size_first, F32) + epsilon)
    step = (target_ratio * jnp.sqrt(ratio)).reshape(1, 1, BI)
    half = step * step / 2.0

    wait_z(10, two_home.at[pl.ds(0, GROUP)])
    wait_y(4, w_home)

    def finish(n, carry):
        r = pl.ds(n * 4, 4)
        out[r] = (ft[r] - step * (one_home[r] + b_home[r])) + half * (two_home[r] + w_home[r])
        return carry

    lax.fori_loop(0, GROUP // 4, finish, 0)
    wait_z(11, two_home.at[pl.ds(GROUP, GROUP)])
    lax.fori_loop(GROUP // 4, BJ // 4, finish, 0)

    for slot in range(16):
        sent = wide.at[0, pl.ds(0, N3 // 2)] if 4 <= slot < 8 else ft.at[pl.ds(0, HALF - 1)]
        pltpu.make_async_copy(sent, sent, zs_sem.at[slot]).wait()
    for slot, rows in ((0, 3 * BJ), (1, 3 * BJ), (2, 3 * GROUP), (3, 3 * GROUP), (4, 3 * BJ)):
        sent = line_f.at[pl.ds(0, rows)]
        pltpu.make_async_copy(sent, sent, ys_sem.at[slot]).wait()
    sent = norm_y.at[pl.ds(0, GY - 1)]
    pltpu.make_async_copy(sent, sent, ns_sem.at[0]).wait()
    sent = norm_all.at[pl.ds(0, GROUP - 1)]
    pltpu.make_async_copy(sent, sent, ns_sem.at[1]).wait()


def on_device(field, factor_a, factor_b, factor_c):
    home = (BJ, BK, BI)
    vmem = pltpu.VMEM
    dma = pltpu.SemaphoreType.DMA
    scratch = [
        vmem(home, F32), vmem((N2, N2), F32), vmem((N3, N3), F32),
        vmem((N1, N1), BF16), vmem((N1, N1), BF16),
        vmem((N2, N2), BF16), vmem((N2, N2), BF16),
        vmem((N3, N3), BF16), vmem((N3, N3), BF16),
        vmem((4, N3, N1), F32), vmem((4, N3, N1), F32), vmem((4, N3, N1), F32),
        vmem((N3, N1), BF16), vmem((N3, N1), BF16),
        vmem(home, F32), vmem(home, F32), vmem(home, F32), vmem(home, F32),
        vmem((N2, KY, BI), F32), vmem((N2, KY, BI), F32),
        vmem((N2, KY, BI), F32), vmem((N2, KY, BI), F32),
        vmem((N2, KY * BI), BF16), vmem((N2, KY * BI), BF16),
        vmem((1, 1, BI), F32), vmem((GY, 1, BI), F32),
        vmem((1, 1, BI), F32), vmem((GROUP, 1, BI), F32),
        dma((6,)), dma((16,)), dma((13,)), dma((5,)), dma((5,)), dma((2,)), dma((2,)),
    ]
    result = pl.pallas_call(
        kernel,
        out_shape=jax.ShapeDtypeStruct(home, F32),
        in_specs=[pl.BlockSpec(memory_space=pltpu.VMEM)] + [pl.BlockSpec(memory_space=pl.ANY)] * 3,
        out_specs=pl.BlockSpec(memory_space=pltpu.VMEM),
        scratch_shapes=scratch,
        compiler_params=pltpu.CompilerParams(
            collective_id=0, has_side_effects=True, vmem_limit_bytes=60 * 1024 * 1024
        ),
        name="taylor",
    )(field, factor_a, factor_b, factor_c)
    return jnp.transpose(result, (1, 2, 0))


def solution(mesh):
    return jax.shard_map(
        on_device, mesh=mesh, in_specs=(P("gz", "gx", "gy"), P(), P(), P()),
        out_specs=P("gz", "gx", "gy"), check_vma=False,
    )
```

```python
import functools

import jax
import jax.numpy as jnp
from jax import lax
from jax.experimental import pallas as pl
from jax.experimental.pallas import tpu as pltpu
from jax.sharding import PartitionSpec as P

MESH = pl.DeviceIdType.MESH
F32, BF16 = jnp.float32, jnp.bfloat16

epsilon = 1e-06
target_ratio = 0.5

GX, GY, GZ = 8, 4, 8
GROUP = GX * GZ
BK, BI, BJ = 32, 128, 128
N1, N2, N3 = 1024, 512, 256
KY = BK // GY
PITCH = BK + 8
PHASES = 2
SIDES = 2
HALF = GROUP // SIDES


def split(x):
    hi = x.astype(BF16)
    return hi, (x - hi.astype(F32)).astype(BF16)


def dot(a, b):
    return jnp.dot(a, b, preferred_element_type=F32)


def dot_t(a, b):
    return lax.dot_general(a, b, (((1,), (1,)), ((), ())), preferred_element_type=F32)


def device_at(z, x, c):
    z, x, c = z % 8, x % 4, c % 2
    return (z // 2) * 2 + c, (z % 2) * 4 + x


def kernel(
    field, a_hbm, b_hbm, c_hbm, out,
    ft, b_f, c_f, a_h, a_l, b_h, b_l, c_h, c_l,
    wide, s_one, s_two, x_h, x_l,
    one_home, two_home, b_home, w_home,
    line_f, line_b, line_s, line_w,
    l_h, l_l, norm_src, norm_y, norm_mid, norm_all,
    load_sem, zs_sem, zr_sem, ys_sem, yr_sem, ns_sem, nr_sem,
):
    gx, gy, gz = lax.axis_index("gx"), lax.axis_index("gy"), lax.axis_index("gz")
    mine = gx * GZ + gz
    z, x, c = (gx // 2) * 2 + gz // 4, gz % 4, gx % 2
    columns = [((x + s // 2) % 4, (c + s) % 2) for s in range(8)]

    def at(z2, s):
        return (z2 // 2) * 2 + columns[s][1], (z2 % 2) * 4 + columns[s][0]

    def all_others(visit):
        def ring(n, carry):
            odd = n % 2
            z2 = (z + 4 + odd * ((n + 1) // 2) - (1 - odd) * (n // 2)) % 8
            for s in range(8):
                visit(*at(z2, s))
            return carry

        lax.fori_loop(0, 7, ring, 0)
        for s in range(1, 8):
            visit(*at(z, s))

    pieces = [(c_hbm, c_f), (b_hbm, b_f)]
    pieces += [(a_hbm.at[pl.ds(n * N3, N3)], s_two.at[n]) for n in range(N1 // N3)]
    loads = [
        pltpu.make_async_copy(src, dst, load_sem.at[n]) for n, (src, dst) in enumerate(pieces)
    ]
    for copy in loads:
        copy.start()

    barrier = pltpu.get_barrier_semaphore()

    def greet(px, pz):
        pl.semaphore_signal(barrier, inc=1, device_id={"gx": px, "gz": pz}, device_id_type=MESH)

    for d in range(1, GY):
        pl.semaphore_signal(
            barrier, inc=1, device_id={"gy": (gy + d) % GY}, device_id_type=MESH
        )
    all_others(greet)

    flat_ft = ft.reshape(BJ * PITCH, BI)

    def turn(k, carry):
        flat_ft[pl.ds(k, BJ, stride=PITCH), :] = field[k].T
        return carry

    lax.fori_loop(0, BK, turn, 0)
    pl.semaphore_wait(barrier, GROUP - 1 + GY - 1)

    def half_ring(sign, send):
        def ring(n, carry):
            for s in range(8):
                send((z + sign * n) % 8, s)
            return carry

        lax.fori_loop(1, 4, ring, 0)
        for s in range(1, 8):
            send(z, s)

    def to_near(p, side):
        sign = 1 - 2 * side

        def place(z2, s):
            px, pz = at(z2, s)
            ox, oz = at((z2 - side) % 8, s)
            src = ft.at[p * GROUP + ox * GZ + oz, pl.ds(0, BK)]
            dst = wide.at[2 * p + side, pl.ds(gz * BK, BK), pl.ds(gx * BI, BI)]
            return px, pz, src, dst

        def send(z2, s):
            px, pz, src, dst = place(z2, s)
            pltpu.make_async_remote_copy(
                src_ref=src, dst_ref=dst,
                send_sem=zs_sem.at[2 * p + side], recv_sem=zr_sem.at[2 * p + side],
                device_id={"gx": px, "gz": pz}, device_id_type=MESH,
            ).start()

        half_ring(sign, send)
        _, _, src, dst = place(z, 0)
        pltpu.make_async_copy(src, dst, zr_sem.at[2 * p + side]).start()

    def swap(p, side):
        sign = 1 - 2 * side
        px, pz = device_at(z + sign, x, c)
        for n in range(4):
            from_z = (z - sign * n) % 8
            rows = pl.ds((from_z % 2) * (N3 // 2), N3 // 2)
            cols = pl.ds((from_z // 2) * (N1 // 4), N1 // 4)
            pltpu.make_async_remote_copy(
                src_ref=wide.at[2 * p + side, rows, cols],
                dst_ref=wide.at[2 * p + 1 - side, rows, cols],
                send_sem=zs_sem.at[4 + 2 * p + side], recv_sem=zr_sem.at[4 + 2 * p + 1 - side],
                device_id={"gx": px, "gz": pz}, device_id_type=MESH,
            ).start()

    def to_home(n, src, dst, p, side, k0=0, depth=BK, late=0):
        sign = 1 - 2 * side
        ox, oz = device_at(z - side, x, c)
        row = p * GROUP + ox * GZ + oz
        target = dst.at[row, pl.ds(k0, depth)]
        arrived = zr_sem.at[8 + 2 * n + p + 3 * late]

        def place(z2, s):
            px, pz = at(z2, s)
            block = src.at[2 * p + side, pl.ds(pz * BK + k0, depth), pl.ds(px * BI, BI)]
            return px, pz, block

        def send(z2, s):
            px, pz, block = place(z2, s)
            pltpu.make_async_remote_copy(
                src_ref=block, dst_ref=target,
                send_sem=zs_sem.at[8 + 4 * n + 2 * p + side], recv_sem=arrived,
                device_id={"gx": px, "gz": pz}, device_id_type=MESH,
            ).start()

        half_ring(-sign, send)
        _, _, block = place(z, 0)
        pltpu.make_async_copy(block, target, arrived).start()

    def wait_z(slot, ref):
        pltpu.make_async_copy(ref, ref, zr_sem.at[slot]).wait()

    def wait_half(slot):
        wait_z(slot, wide.at[0, pl.ds(0, N3 // 2)])

    def to_peer(slot, src, dst, j0, rows, py):
        pltpu.make_async_remote_copy(
            src_ref=src.at[pl.ds(j0, rows), pl.ds(py * KY, KY), :],
            dst_ref=dst.at[pl.ds(gy * BJ + j0, rows)],
            send_sem=ys_sem.at[slot], recv_sem=yr_sem.at[slot],
            device_id={"gy": py}, device_id_type=MESH,
        ).start()

    def to_line(slot, src, dst, j0, rows, peers=(1, 2, 3), own=True):
        for d in peers:
            to_peer(slot, src, dst, j0, rows, (gy + d) % GY)
        if own:
            pltpu.make_async_copy(
                src.at[pl.ds(j0, rows), pl.ds(gy * KY, KY), :],
                dst.at[pl.ds(gy * BJ + j0, rows)],
                yr_sem.at[slot],
            ).start()

    def from_line(slot, src, dst, d):
        py = (gy + d) % GY
        source, target = src.at[pl.ds(py * BJ, BJ)], dst.at[:, pl.ds(gy * KY, KY), :]
        if d:
            pltpu.make_async_remote_copy(
                src_ref=source, dst_ref=target,
                send_sem=ys_sem.at[slot], recv_sem=yr_sem.at[slot],
                device_id={"gy": py}, device_id_type=MESH,
            ).start()
        else:
            pltpu.make_async_copy(source, target, yr_sem.at[slot]).start()

    def wait_y(slot, ref):
        pltpu.make_async_copy(ref, ref, yr_sem.at[slot]).wait()

    for side in range(SIDES):
        to_near(0, side)
    to_line(0, ft, line_f, 0, BJ)
    for side in range(SIDES):
        to_near(1, side)

    for copy in loads:
        copy.wait()
    c_h[...], c_l[...] = split(c_f[...])
    b_h[...], b_l[...] = split(b_f[...])

    def split_a(n, carry):
        rows = pl.ds(pl.multiple_of(n * 128, 128), 128)
        part = pl.ds(pl.multiple_of((n % 2) * 128, 128), 128)
        a_h[rows, :], a_l[rows, :] = split(s_two[n // 2, part, :])
        return carry

    lax.fori_loop(0, N1 // 128, split_a, 0)

    def along_wide(src, dst, p):
        def cut(n, carry):
            rows = pl.ds(pl.multiple_of(n * 64, 64), 64)
            x_h[rows, :], x_l[rows, :] = split(src[p, rows, :])
            return carry

        lax.fori_loop(0, N3 // 64, cut, 0)

        def tile(n, carry):
            cols = pl.ds(pl.multiple_of(n * 256, 256), 256)
            a_hi, a_lo = a_h[cols, :], a_l[cols, :]
            total = dot_t(x_h[...], a_hi) + dot_t(x_l[...], a_hi) + dot_t(x_h[...], a_lo)
            xh, xl = x_h[:, cols], x_l[:, cols]
            total = total + dot(c_h[...], xh) + dot(c_l[...], xh) + dot(c_h[...], xl)
            dst[p, :, cols] = total
            return carry

        lax.fori_loop(0, N1 // 256, tile, 0)

    def cut_line(src, j0, rows):
        flat = src.reshape(N2 * KY, BI)
        to = pl.ds(j0, rows)

        def one(k, carry):
            cols = pl.ds(pl.multiple_of(k * BI, BI), BI)
            l_h[to, cols], l_l[to, cols] = split(flat[pl.ds(j0 * KY + k, rows, stride=KY), :])
            return carry

        lax.fori_loop(0, KY, one, 0)

    def line_rows(d, dst, add):
        j0 = pl.multiple_of((gy + d) % GY * BJ, BJ)
        flat = dst.reshape(N2 * KY, BI)
        b_hi, b_lo = b_h[pl.ds(j0, BJ), :], b_l[pl.ds(j0, BJ), :]

        def pair(q, carry):
            cols = pl.ds(pl.multiple_of(q * 2 * BI, 2 * BI), 2 * BI)
            xh, xl = l_h[:, cols], l_l[:, cols]
            total = dot(b_hi, xh) + dot(b_hi, xl) + dot(b_lo, xh)
            for e in range(2):
                rows = pl.ds(j0 * KY + 2 * q + e, BJ, stride=KY)
                part = total[:, e * BI:(e + 1) * BI]
                flat[rows, :] = flat[rows, :] + 2.0 * part if add else part
            return carry

        lax.fori_loop(0, KY // 2, pair, 0)

    for side in range(SIDES):
        wait_half(side)
        swap(0, side)

    wait_y(0, line_f)
    cut_line(line_f, 0, N2)
    for d in (1, 2, 3, 0):
        line_rows(d, line_b, False)
        from_line(1, line_b, b_home, d)

    for side in range(SIDES):
        wait_half(2 + side)
        swap(1, side)

    cut_line(line_b, 0, N2)
    for d in range(GY):
        line_rows(d, line_w, False)

    k_early, k_late = (1 - gy // 2) * (BK // 2), (gy // 2) * (BK // 2)
    for side in range(SIDES):
        wait_half(4 + side)
        along_wide(wide, s_one, side)
        to_home(0, s_one, one_home, 0, side)
    for side in range(SIDES):
        wait_half(6 + side)
        along_wide(wide, s_one, 2 + side)
    for side in range(SIDES):
        to_home(0, s_one, one_home, 1, side, k_early, BK // 2)
    for side in range(SIDES):
        to_home(0, s_one, one_home, 1, side, k_late, BK // 2, late=1)
    for side in range(SIDES):
        along_wide(s_one, s_two, side)
        to_home(1, s_two, two_home, 0, side)

    wait_z(8, one_home.at[pl.ds(0, GROUP)])
    to_line(2, one_home, line_s, 0, GROUP)

    for side in range(SIDES):
        along_wide(s_one, s_two, 2 + side)

    def squares(read):
        def add(n, carry):
            v = read(pl.ds(n * 8, 8))
            return carry + jnp.sum(v * v, axis=(0, 1)).reshape(1, BI)

        return add

    zero = jnp.zeros((1, BI), F32)
    of_field = lax.fori_loop(0, BJ // 8, squares(lambda r: ft[r, pl.ds(0, BK)]), zero)
    wait_y(1, b_home)
    first = squares(lambda r: one_home[r] + b_home[r])
    of_first = lax.fori_loop(0, GROUP // 8, first, zero)

    half_phase = one_home.at[pl.ds(0, GROUP), pl.ds(0, BK // 2)]
    wait_z(9, half_phase)
    for tile in range(2):
        py = (1 - gy // 2) * 2 + tile
        to_peer(3, one_home, line_s, GROUP, GROUP, py)
    wait_z(12, half_phase)
    to_peer(3, one_home, line_s, GROUP, GROUP, gy + 1 - 2 * (gy % 2))
    to_line(3, one_home, line_s, GROUP, GROUP, peers=())
    of_first = lax.fori_loop(GROUP // 8, BJ // 8, first, of_first)

    lane = lax.broadcasted_iota(jnp.int32, (1, BI), 1)
    norm_src[0] = jnp.where(lane == 0, jnp.sum(of_field), jnp.sum(of_first))

    def send_norm_y():
        for d in range(1, GY):
            pltpu.make_async_remote_copy(
                src_ref=norm_src, dst_ref=norm_y.at[pl.ds(gy, 1)],
                send_sem=ns_sem.at[0], recv_sem=nr_sem.at[0],
                device_id={"gy": (gy + d) % GY}, device_id_type=MESH,
            ).start()
        pltpu.make_async_copy(norm_src, norm_y.at[pl.ds(gy, 1)], nr_sem.at[0]).start()

    send_norm_y()
    for side in range(SIDES):
        to_home(1, s_two, two_home, 1, side)
    wait_y(2, line_s.at[pl.ds(0, N2 // 2)])
    for d in range(GY):
        cut_line(line_s, d * BJ, GROUP)
    wait_y(3, line_s.at[pl.ds(0, N2 // 2)])
    for d in range(GY):
        cut_line(line_s, d * BJ + GROUP, GROUP)
    for d in (2, 1, 3, 0):
        line_rows(d, line_w, True)
        from_line(4, line_w, w_home, d)

    pltpu.make_async_copy(norm_y, norm_y, nr_sem.at[0]).wait()
    norm_mid[0] = norm_y[0] + norm_y[1] + norm_y[2] + norm_y[3]

    def send_norm(px, pz):
        pltpu.make_async_remote_copy(
            src_ref=norm_mid, dst_ref=norm_all.at[pl.ds(mine, 1)],
            send_sem=ns_sem.at[1], recv_sem=nr_sem.at[1],
            device_id={"gx": px, "gz": pz}, device_id_type=MESH,
        ).start()

    all_others(send_norm)
    pltpu.make_async_copy(norm_mid, norm_all.at[pl.ds(mine, 1)], nr_sem.at[1]).start()

    pltpu.make_async_copy(norm_all, norm_all, nr_sem.at[1]).wait()
    sums = jnp.sum(norm_all[...], axis=0)
    size_field = jnp.sum(jnp.where(lane == 0, sums, 0.0))
    size_first = jnp.sum(jnp.where(lane == 1, sums, 0.0))
    ratio = jnp.full((1, BI), size_field, F32) / (jnp.full((1, BI), size_first, F32) + epsilon)
    step = (target_ratio * jnp.sqrt(ratio)).reshape(1, 1, BI)
    half = step * step / 2.0

    wait_z(10, two_home.at[pl.ds(0, GROUP)])
    wait_y(4, w_home)

    def finish(n, carry):
        r = pl.ds(n * 4, 4)
        out[r] = (ft[r, pl.ds(0, BK)] - step * (one_home[r] + b_home[r])) + half * (two_home[r] + w_home[r])
        return carry

    lax.fori_loop(0, GROUP // 4, finish, 0)
    wait_z(11, two_home.at[pl.ds(GROUP, GROUP)])
    lax.fori_loop(GROUP // 4, BJ // 4, finish, 0)

    for slot in range(16):
        sent = wide.at[0, pl.ds(0, N3 // 2)] if 4 <= slot < 8 else one_home.at[pl.ds(0, HALF - 1)]
        pltpu.make_async_copy(sent, sent, zs_sem.at[slot]).wait()
    for slot, rows in ((0, 3 * BJ), (1, 3 * BJ), (2, 3 * GROUP), (3, 3 * GROUP), (4, 3 * BJ)):
        sent = line_f.at[pl.ds(0, rows)]
        pltpu.make_async_copy(sent, sent, ys_sem.at[slot]).wait()
    sent = norm_y.at[pl.ds(0, GY - 1)]
    pltpu.make_async_copy(sent, sent, ns_sem.at[0]).wait()
    sent = norm_all.at[pl.ds(0, GROUP - 1)]
    pltpu.make_async_copy(sent, sent, ns_sem.at[1]).wait()


def on_device(field, factor_a, factor_b, factor_c):
    home = (BJ, BK, BI)
    vmem = pltpu.VMEM
    dma = pltpu.SemaphoreType.DMA
    scratch = [
        vmem((BJ, PITCH, BI), F32), vmem((N2, N2), F32), vmem((N3, N3), F32),
        vmem((N1, N1), BF16), vmem((N1, N1), BF16),
        vmem((N2, N2), BF16), vmem((N2, N2), BF16),
        vmem((N3, N3), BF16), vmem((N3, N3), BF16),
        vmem((4, N3, N1), F32), vmem((4, N3, N1), F32), vmem((4, N3, N1), F32),
        vmem((N3, N1), BF16), vmem((N3, N1), BF16),
        vmem(home, F32), vmem(home, F32), vmem(home, F32), vmem(home, F32),
        vmem((N2, KY, BI), F32), vmem((N2, KY, BI), F32),
        vmem((N2, KY, BI), F32), vmem((N2, KY, BI), F32),
        vmem((N2, KY * BI), BF16), vmem((N2, KY * BI), BF16),
        vmem((1, 1, BI), F32), vmem((GY, 1, BI), F32),
        vmem((1, 1, BI), F32), vmem((GROUP, 1, BI), F32),
        dma((6,)), dma((16,)), dma((13,)), dma((5,)), dma((5,)), dma((2,)), dma((2,)),
    ]
    result = pl.pallas_call(
        kernel,
        out_shape=jax.ShapeDtypeStruct(home, F32),
        in_specs=[pl.BlockSpec(memory_space=pltpu.VMEM)] + [pl.BlockSpec(memory_space=pl.ANY)] * 3,
        out_specs=pl.BlockSpec(memory_space=pltpu.VMEM),
        scratch_shapes=scratch,
        compiler_params=pltpu.CompilerParams(
            collective_id=0, has_side_effects=True, vmem_limit_bytes=60 * 1024 * 1024
        ),
        name="taylor",
    )(field, factor_a, factor_b, factor_c)
    return jnp.transpose(result, (1, 2, 0))


def solution(mesh):
    return jax.shard_map(
        on_device, mesh=mesh, in_specs=(P("gz", "gx", "gy"), P(), P(), P()),
        out_specs=P("gz", "gx", "gy"), check_vma=False,
    )
```

```python
import functools

import jax
import jax.numpy as jnp
from jax import lax
from jax.experimental import pallas as pl
from jax.experimental.pallas import tpu as pltpu
from jax.sharding import PartitionSpec as P

MESH = pl.DeviceIdType.MESH
F32, BF16 = jnp.float32, jnp.bfloat16

epsilon = 1e-06
target_ratio = 0.5

GX, GY, GZ = 8, 4, 8
GROUP = GX * GZ
BK, BI, BJ = 32, 128, 128
N1, N2, N3 = 1024, 512, 256
KY = BK // GY
PITCH = BK + 8
PHASES = 2
SIDES = 2
HALF = GROUP // SIDES


def split(x):
    hi = x.astype(BF16)
    return hi, (x - hi.astype(F32)).astype(BF16)


def dot(a, b):
    return jnp.dot(a, b, preferred_element_type=F32)


def dot_t(a, b):
    return lax.dot_general(a, b, (((1,), (1,)), ((), ())), preferred_element_type=F32)


def device_at(z, x, c):
    z, x, c = z % 8, x % 4, c % 2
    return (z // 2) * 2 + c, (z % 2) * 4 + x


def kernel(
    field_hbm, a_hbm, b_hbm, c_hbm, out,
    field, ft, b_f, c_f, a_h, a_l, b_h, b_l, c_h, c_l,
    wide, s_one, s_two, x_h, x_l,
    one_home, two_home, b_home, w_home,
    line_f, line_b, line_s, line_w,
    l_h, l_l, norm_src, norm_y, norm_mid, norm_all,
    load_sem, zs_sem, zr_sem, ys_sem, yr_sem, ns_sem, nr_sem,
):
    gx, gy, gz = lax.axis_index("gx"), lax.axis_index("gy"), lax.axis_index("gz")
    mine = gx * GZ + gz
    z, x, c = (gx // 2) * 2 + gz // 4, gz % 4, gx % 2
    columns = [((x + s // 2) % 4, (c + s) % 2) for s in range(8)]

    def at(z2, s):
        return (z2 // 2) * 2 + columns[s][1], (z2 % 2) * 4 + columns[s][0]

    def all_others(visit):
        def ring(n, carry):
            odd = n % 2
            z2 = (z + 4 + odd * ((n + 1) // 2) - (1 - odd) * (n // 2)) % 8
            for s in range(8):
                visit(*at(z2, s))
            return carry

        lax.fori_loop(0, 7, ring, 0)
        for s in range(1, 8):
            visit(*at(z, s))

    pieces = [(c_hbm, c_f), (b_hbm, b_f)]
    pieces += [(a_hbm.at[pl.ds(n * N3, N3)], s_two.at[n]) for n in range(N1 // N3)]
    loads = [
        pltpu.make_async_copy(src, dst, load_sem.at[n]) for n, (src, dst) in enumerate(pieces)
    ]
    field_load = pltpu.make_async_copy(field_hbm, field, load_sem.at[6])
    field_load.start()

    barrier = pltpu.get_barrier_semaphore()

    def greet(px, pz):
        pl.semaphore_signal(barrier, inc=1, device_id={"gx": px, "gz": pz}, device_id_type=MESH)

    for d in range(1, GY):
        pl.semaphore_signal(
            barrier, inc=1, device_id={"gy": (gy + d) % GY}, device_id_type=MESH
        )
    all_others(greet)

    flat_ft = ft.reshape(BJ * PITCH, BI)

    def turn(k, carry):
        flat_ft[pl.ds(k, BJ, stride=PITCH), :] = field[k].T
        return carry

    field_load.wait()
    for copy in loads:
        copy.start()
    lax.fori_loop(0, BK, turn, 0)
    pl.semaphore_wait(barrier, GROUP - 1 + GY - 1)

    def half_ring(sign, send):
        def ring(n, carry):
            for s in range(8):
                send((z + sign * (4 - n)) % 8, s)
            return carry

        lax.fori_loop(1, 4, ring, 0)
        for s in range(1, 8):
            send(z, s)

    def to_near(p, side):
        sign = 1 - 2 * side

        def place(z2, s):
            px, pz = at(z2, s)
            ox, oz = at((z2 - side) % 8, s)
            src = ft.at[p * GROUP + ox * GZ + oz, pl.ds(0, BK)]
            dst = wide.at[2 * p + side, pl.ds(gz * BK, BK), pl.ds(gx * BI, BI)]
            return px, pz, src, dst

        def send(z2, s):
            px, pz, src, dst = place(z2, s)
            pltpu.make_async_remote_copy(
                src_ref=src, dst_ref=dst,
                send_sem=zs_sem.at[2 * p + side], recv_sem=zr_sem.at[2 * p + side],
                device_id={"gx": px, "gz": pz}, device_id_type=MESH,
            ).start()

        half_ring(sign, send)
        _, _, src, dst = place(z, 0)
        pltpu.make_async_copy(src, dst, zr_sem.at[2 * p + side]).start()

    def swap(p, side):
        sign = 1 - 2 * side
        px, pz = device_at(z + sign, x, c)
        for n in range(4):
            from_z = (z - sign * n) % 8
            rows = pl.ds((from_z % 2) * (N3 // 2), N3 // 2)
            cols = pl.ds((from_z // 2) * (N1 // 4), N1 // 4)
            pltpu.make_async_remote_copy(
                src_ref=wide.at[2 * p + side, rows, cols],
                dst_ref=wide.at[2 * p + 1 - side, rows, cols],
                send_sem=zs_sem.at[4 + 2 * p + side], recv_sem=zr_sem.at[4 + 2 * p + 1 - side],
                device_id={"gx": px, "gz": pz}, device_id_type=MESH,
            ).start()

    def to_home(n, src, dst, p, side, k0=0, depth=BK, late=0):
        sign = 1 - 2 * side
        ox, oz = device_at(z - side, x, c)
        row = p * GROUP + ox * GZ + oz
        target = dst.at[row, pl.ds(k0, depth)]
        arrived = zr_sem.at[13 + late - 2 * p if late else 8 + 2 * n + p]

        def place(z2, s):
            px, pz = at(z2, s)
            block = src.at[2 * p + side, pl.ds(pz * BK + k0, depth), pl.ds(px * BI, BI)]
            return px, pz, block

        def send(z2, s):
            px, pz, block = place(z2, s)
            pltpu.make_async_remote_copy(
                src_ref=block, dst_ref=target,
                send_sem=zs_sem.at[8 + 4 * n + 2 * p + side], recv_sem=arrived,
                device_id={"gx": px, "gz": pz}, device_id_type=MESH,
            ).start()

        half_ring(-sign, send)
        _, _, block = place(z, 0)
        pltpu.make_async_copy(block, target, arrived).start()

    def wait_z(slot, ref):
        pltpu.make_async_copy(ref, ref, zr_sem.at[slot]).wait()

    def wait_half(slot):
        wait_z(slot, wide.at[0, pl.ds(0, N3 // 2)])

    def to_peer(slot, src, dst, j0, rows, py):
        pltpu.make_async_remote_copy(
            src_ref=src.at[pl.ds(j0, rows), pl.ds(py * KY, KY), :],
            dst_ref=dst.at[pl.ds(gy * BJ + j0, rows)],
            send_sem=ys_sem.at[slot], recv_sem=yr_sem.at[slot],
            device_id={"gy": py}, device_id_type=MESH,
        ).start()

    def to_line(slot, src, dst, j0, rows, peers=(1, 2, 3), own=True):
        for d in peers:
            to_peer(slot, src, dst, j0, rows, (gy + d) % GY)
        if own:
            pltpu.make_async_copy(
                src.at[pl.ds(j0, rows), pl.ds(gy * KY, KY), :],
                dst.at[pl.ds(gy * BJ + j0, rows)],
                yr_sem.at[slot],
            ).start()

    def from_line(slot, src, dst, d):
        py = (gy + d) % GY
        source, target = src.at[pl.ds(py * BJ, BJ)], dst.at[:, pl.ds(gy * KY, KY), :]
        if d:
            pltpu.make_async_remote_copy(
                src_ref=source, dst_ref=target,
                send_sem=ys_sem.at[slot], recv_sem=yr_sem.at[slot],
                device_id={"gy": py}, device_id_type=MESH,
            ).start()
        else:
            pltpu.make_async_copy(source, target, yr_sem.at[slot]).start()

    def wait_y(slot, ref):
        pltpu.make_async_copy(ref, ref, yr_sem.at[slot]).wait()

    for side in range(SIDES):
        to_near(0, side)
    to_line(0, ft, line_f, 0, BJ)
    for side in range(SIDES):
        to_near(1, side)

    for copy in loads:
        copy.wait()
    c_h[...], c_l[...] = split(c_f[...])
    b_h[...], b_l[...] = split(b_f[...])

    def split_a(n, carry):
        rows = pl.ds(pl.multiple_of(n * 128, 128), 128)
        part = pl.ds(pl.multiple_of((n % 2) * 128, 128), 128)
        a_h[rows, :], a_l[rows, :] = split(s_two[n // 2, part, :])
        return carry

    lax.fori_loop(0, N1 // 128, split_a, 0)

    def along_wide(src, dst, p):
        def cut(n, carry):
            rows = pl.ds(pl.multiple_of(n * 64, 64), 64)
            x_h[rows, :], x_l[rows, :] = split(src[p, rows, :])
            return carry

        lax.fori_loop(0, N3 // 64, cut, 0)

        def tile(n, carry):
            cols = pl.ds(pl.multiple_of(n * 256, 256), 256)
            a_hi, a_lo = a_h[cols, :], a_l[cols, :]
            total = dot_t(x_h[...], a_hi) + dot_t(x_l[...], a_hi) + dot_t(x_h[...], a_lo)
            xh, xl = x_h[:, cols], x_l[:, cols]
            total = total + dot(c_h[...], xh) + dot(c_l[...], xh) + dot(c_h[...], xl)
            dst[p, :, cols] = total
            return carry

        lax.fori_loop(0, N1 // 256, tile, 0)

    def cut_line(src, j0, rows):
        flat = src.reshape(N2 * KY, BI)
        to = pl.ds(j0, rows)

        def one(k, carry):
            cols = pl.ds(pl.multiple_of(k * BI, BI), BI)
            l_h[to, cols], l_l[to, cols] = split(flat[pl.ds(j0 * KY + k, rows, stride=KY), :])
            return carry

        lax.fori_loop(0, KY, one, 0)

    def line_rows(d, dst, add):
        j0 = pl.multiple_of((gy + d) % GY * BJ, BJ)
        flat = dst.reshape(N2 * KY, BI)
        b_hi, b_lo = b_h[pl.ds(j0, BJ), :], b_l[pl.ds(j0, BJ), :]

        def pair(q, carry):
            cols = pl.ds(pl.multiple_of(q * 2 * BI, 2 * BI), 2 * BI)
            xh, xl = l_h[:, cols], l_l[:, cols]
            total = dot(b_hi, xh) + dot(b_hi, xl) + dot(b_lo, xh)
            for e in range(2):
                rows = pl.ds(j0 * KY + 2 * q + e, BJ, stride=KY)
                part = total[:, e * BI:(e + 1) * BI]
                flat[rows, :] = flat[rows, :] + 2.0 * part if add else part
            return carry

        lax.fori_loop(0, KY // 2, pair, 0)

    for side in range(SIDES):
        wait_half(side)
        swap(0, side)

    wait_y(0, line_f)
    cut_line(line_f, 0, N2)
    for d in (1, 2, 3, 0):
        line_rows(d, line_b, False)
        from_line(1, line_b, b_home, d)

    for side in range(SIDES):
        wait_half(2 + side)
        swap(1, side)

    cut_line(line_b, 0, N2)
    for d in range(GY):
        line_rows(d, line_w, False)

    mate = gy + 1 - 2 * (gy % 2)
    k_early = (1 - gy // 2) * (BK // 2)
    parts = ((k_early, BK // 2, 0), (mate * KY, KY, 1), (gy * KY, KY, 2))
    for p in range(PHASES):
        for side in range(SIDES):
            wait_half(4 + 2 * p + side)
            along_wide(wide, s_one, 2 * p + side)
        for k0, depth, late in parts:
            for side in range(SIDES):
                to_home(0, s_one, one_home, p, side, k0, depth, late)
    for side in range(SIDES):
        along_wide(s_one, s_two, side)
        to_home(1, s_two, two_home, 0, side)

    def forward(p):
        wait_z(8 + p, one_home.at[pl.ds(0, GROUP), pl.ds(0, BK // 2)])
        for tile in range(2):
            to_peer(2 + p, one_home, line_s, p * GROUP, GROUP, (1 - gy // 2) * 2 + tile)
        wait_z(14 - 2 * p, one_home.at[pl.ds(0, GROUP), pl.ds(0, KY)])
        to_peer(2 + p, one_home, line_s, p * GROUP, GROUP, mate)
        wait_z(15 - 2 * p, one_home.at[pl.ds(0, GROUP), pl.ds(0, KY)])
        to_line(2 + p, one_home, line_s, p * GROUP, GROUP, peers=())

    forward(0)

    for side in range(SIDES):
        along_wide(s_one, s_two, 2 + side)

    def squares(read):
        def add(n, carry):
            v = read(pl.ds(n * 8, 8))
            return carry + jnp.sum(v * v, axis=(0, 1)).reshape(1, BI)

        return add

    zero = jnp.zeros((1, BI), F32)
    of_field = lax.fori_loop(0, BJ // 8, squares(lambda r: ft[r, pl.ds(0, BK)]), zero)
    wait_y(1, b_home)
    first = squares(lambda r: one_home[r] + b_home[r])
    of_first = lax.fori_loop(0, GROUP // 8, first, zero)

    forward(1)
    of_first = lax.fori_loop(GROUP // 8, BJ // 8, first, of_first)

    lane = lax.broadcasted_iota(jnp.int32, (1, BI), 1)
    norm_src[0] = jnp.where(lane == 0, jnp.sum(of_field), jnp.sum(of_first))

    def send_norm_y():
        for d in range(1, GY):
            pltpu.make_async_remote_copy(
                src_ref=norm_src, dst_ref=norm_y.at[pl.ds(gy, 1)],
                send_sem=ns_sem.at[0], recv_sem=nr_sem.at[0],
                device_id={"gy": (gy + d) % GY}, device_id_type=MESH,
            ).start()
        pltpu.make_async_copy(norm_src, norm_y.at[pl.ds(gy, 1)], nr_sem.at[0]).start()

    send_norm_y()
    wait_y(2, line_s.at[pl.ds(0, N2 // 2)])
    for d in range(GY):
        cut_line(line_s, d * BJ, GROUP)
    wait_y(3, line_s.at[pl.ds(0, N2 // 2)])
    for d in range(GY):
        cut_line(line_s, d * BJ + GROUP, GROUP)
    line_rows(2, line_w, True)
    from_line(4, line_w, w_home, 2)

    pltpu.make_async_copy(norm_y, norm_y, nr_sem.at[0]).wait()
    norm_mid[0] = norm_y[0] + norm_y[1] + norm_y[2] + norm_y[3]

    def send_norm(px, pz):
        pltpu.make_async_remote_copy(
            src_ref=norm_mid, dst_ref=norm_all.at[pl.ds(mine, 1)],
            send_sem=ns_sem.at[1], recv_sem=nr_sem.at[1],
            device_id={"gx": px, "gz": pz}, device_id_type=MESH,
        ).start()

    all_others(send_norm)
    pltpu.make_async_copy(norm_mid, norm_all.at[pl.ds(mine, 1)], nr_sem.at[1]).start()
    for side in range(SIDES):
        to_home(1, s_two, two_home, 1, side)

    for d in (1, 3, 0):
        line_rows(d, line_w, True)
        from_line(4, line_w, w_home, d)

    pltpu.make_async_copy(norm_all, norm_all, nr_sem.at[1]).wait()
    sums = jnp.sum(norm_all[...], axis=0)
    size_field = jnp.sum(jnp.where(lane == 0, sums, 0.0))
    size_first = jnp.sum(jnp.where(lane == 1, sums, 0.0))
    ratio = jnp.full((1, BI), size_field, F32) / (jnp.full((1, BI), size_first, F32) + epsilon)
    step = (target_ratio * jnp.sqrt(ratio)).reshape(1, 1, BI)
    half = step * step / 2.0

    wait_z(10, two_home.at[pl.ds(0, GROUP)])
    wait_y(4, w_home)

    def finish(n, carry):
        r = pl.ds(n * 4, 4)
        out[r] = (ft[r, pl.ds(0, BK)] - step * (one_home[r] + b_home[r])) + half * (two_home[r] + w_home[r])
        return carry

    lax.fori_loop(0, GROUP // 4, finish, 0)
    wait_z(11, two_home.at[pl.ds(GROUP, GROUP)])
    lax.fori_loop(GROUP // 4, BJ // 4, finish, 0)

    for slot in range(16):
        sent = wide.at[0, pl.ds(0, N3 // 2)] if 4 <= slot < 8 else one_home.at[pl.ds(0, HALF - 1)]
        pltpu.make_async_copy(sent, sent, zs_sem.at[slot]).wait()
    for slot, rows in ((0, 3 * BJ), (1, 3 * BJ), (2, 3 * GROUP), (3, 3 * GROUP), (4, 3 * BJ)):
        sent = line_f.at[pl.ds(0, rows)]
        pltpu.make_async_copy(sent, sent, ys_sem.at[slot]).wait()
    sent = norm_y.at[pl.ds(0, GY - 1)]
    pltpu.make_async_copy(sent, sent, ns_sem.at[0]).wait()
    sent = norm_all.at[pl.ds(0, GROUP - 1)]
    pltpu.make_async_copy(sent, sent, ns_sem.at[1]).wait()


def on_device(field, factor_a, factor_b, factor_c):
    home = (BJ, BK, BI)
    vmem = pltpu.VMEM
    dma = pltpu.SemaphoreType.DMA
    scratch = [
        vmem((BK, BI, BJ), F32), vmem((BJ, PITCH, BI), F32), vmem((N2, N2), F32), vmem((N3, N3), F32),
        vmem((N1, N1), BF16), vmem((N1, N1), BF16),
        vmem((N2, N2), BF16), vmem((N2, N2), BF16),
        vmem((N3, N3), BF16), vmem((N3, N3), BF16),
        vmem((4, N3, N1), F32), vmem((4, N3, N1), F32), vmem((4, N3, N1), F32),
        vmem((N3, N1), BF16), vmem((N3, N1), BF16),
        vmem(home, F32), vmem(home, F32), vmem(home, F32), vmem(home, F32),
        vmem((N2, KY, BI), F32), vmem((N2, KY, BI), F32),
        vmem((N2, KY, BI), F32), vmem((N2, KY, BI), F32),
        vmem((N2, KY * BI), BF16), vmem((N2, KY * BI), BF16),
        vmem((1, 1, BI), F32), vmem((GY, 1, BI), F32),
        vmem((1, 1, BI), F32), vmem((GROUP, 1, BI), F32),
        dma((7,)), dma((16,)), dma((16,)), dma((5,)), dma((5,)), dma((2,)), dma((2,)),
    ]
    result = pl.pallas_call(
        kernel,
        out_shape=jax.ShapeDtypeStruct(home, F32),
        in_specs=[pl.BlockSpec(memory_space=pl.ANY)] * 4,
        out_specs=pl.BlockSpec(memory_space=pltpu.VMEM),
        scratch_shapes=scratch,
        compiler_params=pltpu.CompilerParams(
            collective_id=0, has_side_effects=True, vmem_limit_bytes=60 * 1024 * 1024
        ),
        name="taylor",
    )(field, factor_a, factor_b, factor_c)
    return jnp.transpose(result, (1, 2, 0))


def solution(mesh):
    return jax.shard_map(
        on_device, mesh=mesh, in_specs=(P("gz", "gx", "gy"), P(), P(), P()),
        out_specs=P("gz", "gx", "gy"), check_vma=False,
    )
```
